32 devices in a mesh: dom: 16 (over z, y, core), sub: 2 (over x).
Axes of the slice: x: 2, y: 2, z: 4, core: 2. Of those that a mesh axis runs over, the one named last changes fastest.
Arguments:
- dofs: float32 [9, 56, 512], P(None, None, ('dom', 'sub')), may hold values from -6 to 6
- stiffness: float32 [3, 56, 56], replicated, may hold values from -0.75 to 0.75
- projection: float32 [4, 21, 56], replicated, may hold values from -0.75 to 0.75
- star: float32 [3, 9, 9, 512], P(None, None, None, ('dom', 'sub')), may hold values from -1.25 to 1.25
- flux_minus: float32 [4, 9, 9, 512], P(None, None, None, ('dom', 'sub')), may hold values from -1 to 1
- flux_plus: float32 [4, 9, 9, 512], P(None, None, None, ('dom', 'sub')), may hold values from -1 to 1
- fault_flux: float32 [9, 9], replicated, may hold values from -2 to 2
- fault_faces: int32 [4, 512], P(None, ('dom', 'sub')), may hold values 0 or 1
- levels: int32 [512], P(('dom', 'sub')), may hold values from 0 to 1, as said below
- face_source: int32 [4, 512], P(None, ('dom', 'sub')), may hold values from 0 to 87, as said below
- send_source: int32 [128], P(('dom', 'sub')), may hold values from 0 to 63
Outputs:
- dofs_after: float32 [9, 56, 512], P(None, None, ('dom', 'sub'))
The draws below stay inside these ranges and needn't reach their ends.
Inputs may be any that keep to these rules, and one draw needn't show every extreme that they name: `levels`: on every device at most 8 of its 16 elements have level 0, and some device has exactly 8. `face_source`: values below 64 name a face of the same device as face times 16 plus element; larger values name received exported faces as defined in the reference program.
All inputs are finite; a program needn't handle non-finite values. No bound on the sum of `fault_faces` on one device may be relied on, other than what follows from the above.
Results may differ from the reference program's by a relative error of at most 0.0001.
Values sent between devices are 32-bit elements; how exact they have to be, the bound alone decides.
A program may use at most 64 MiB of HBM per device.

```python
import math
import jax
import jax.numpy as jnp
from jax import lax

VARS = 9
MODES = 56
FACE_MODES = 21
ORDER = 6
E_DEV = 16
SEND = 4
FINE_MOST = 8
RECV = 24
ELEMS = 512
N_DOM = 16
N_SUB = 2
DEVICES = 32


def draw_levels(key, part):
    device_count = ELEMS // E_DEV
    key_count, key_busiest, key_ranks = jax.random.split(key, 3)
    counts = jax.random.randint(key_count, (device_count,), FINE_MOST // 4, FINE_MOST + 1)
    busiest = jax.random.randint(key_busiest, (), 0, device_count)
    counts = jnp.where(jnp.arange(device_count) == busiest, FINE_MOST, counts)
    ranks = jax.vmap(lambda single: jax.random.permutation(single, E_DEV))(jax.random.split(key_ranks, device_count))
    return jnp.where(ranks < counts[:, None], 0, 1).astype(jnp.int32).reshape(-1)


def draw_face_source(key, part):
    key_kind, key_local, key_remote = jax.random.split(key, 3)
    grid_shape = (4, ELEMS)
    choose_kind = jax.random.randint(key_kind, grid_shape, 0, 4)
    local_codes = jax.random.randint(key_local, grid_shape, 0, 4 * E_DEV)
    remote_codes = 4 * E_DEV + jax.random.randint(key_remote, grid_shape, 0, RECV)
    return jnp.where(choose_kind < 3, local_codes, remote_codes).astype(jnp.int32)


def touch_ends(result, key, least, high):
    extent = result.shape
    index_at = [jax.random.randint(jax.random.fold_in(key, axis), (), 0, extent[axis]) for axis in range(len(extent))]
    result = result.at[tuple(index_at)].set(least)
    longest = extent.index(max(extent))
    index_at[longest] = (index_at[longest] + 1) % extent[longest]
    return result.at[tuple(index_at)].set(high)


def block_scale(key, shape, cuts, least, largest):
    gain = 1.0
    for dim, blocks in cuts:
        heights = jax.random.uniform(jax.random.fold_in(jax.random.fold_in(key, 6), dim), (blocks,), jnp.float32, least / len(cuts), largest / len(cuts))
        gain = gain * jnp.repeat(jnp.exp(heights), shape[dim] // blocks).reshape((-1,) + (1,) * (len(shape) - 1 - dim))
    return gain


def bell_draw(stream_key, extent, width, most, cuts=(), kind=jnp.bfloat16):
    values = width * jax.random.normal(stream_key, extent, jnp.float32)
    if cuts:
        values = values * block_scale(stream_key, extent, cuts, -0.22, 0.18)
    return jnp.clip(values, -most, most).astype(kind)


def setup_inputs(seed: int = 0) -> dict:
    arg_keys = jax.random.split(jax.random.key(seed), 12)
    dofs = bell_draw(arg_keys[0], (VARS, MODES, ELEMS), 1.0, 6.0, ((2, 32),), jnp.float32)
    stiffness = bell_draw(arg_keys[1], (3, MODES, MODES), MODES ** -0.5, 0.75, (), jnp.float32)
    projection = bell_draw(arg_keys[2], (4, FACE_MODES, MODES), MODES ** -0.5, 0.75, (), jnp.float32)
    star = bell_draw(arg_keys[3], (3, VARS, VARS, ELEMS), 27 ** -0.5, 1.25, ((3, 32),), jnp.float32)
    flux_minus = bell_draw(arg_keys[4], (4, VARS, VARS, ELEMS), 36 ** -0.5, 1.0, ((3, 32),), jnp.float32)
    flux_plus = bell_draw(arg_keys[5], (4, VARS, VARS, ELEMS), 36 ** -0.5, 1.0, ((3, 32),), jnp.float32)
    fault_flux = bell_draw(arg_keys[6], (VARS, VARS), 9 ** -0.5, 2.0, (), jnp.float32)
    fault_faces = touch_ends((jax.random.randint(arg_keys[7], (4, ELEMS), 0, 8) < 1).astype(jnp.int32), jax.random.fold_in(arg_keys[7], 1), 0, 1)
    levels = draw_levels(jax.random.fold_in(arg_keys[11], 71), 0)
    face_source = draw_face_source(jax.random.fold_in(arg_keys[11], 71), 0)
    send_source = touch_ends(jax.random.randint(arg_keys[10], (SEND * DEVICES,), 0, 4 * E_DEV), jax.random.fold_in(arg_keys[10], 1), 0, (4 * E_DEV) - 1).astype(jnp.int32)
    return dict(dofs=dofs, stiffness=stiffness, projection=projection, star=star, flux_minus=flux_minus, flux_plus=flux_plus, fault_flux=fault_flux, fault_faces=fault_faces, levels=levels, face_source=face_source, send_source=send_source)


fine_step = 0.75
exact_reference = lax.Precision.HIGHEST


def taylor_weights(start_time, stop_time, term_count):
    return [(stop_time ** (term + 1) - start_time ** (term + 1)) / math.factorial(term + 1) for term in range(term_count)]


def derivatives(state_now, stiffness, star_contribution):
    taylor_series = [state_now]
    for repeat in range(ORDER - 1):
        time_slopes = jnp.einsum("dmn,wne->dwme", stiffness, taylor_series[-1], precision=exact_reference)
        taylor_series.append(jnp.einsum("usij,uifj->sfj", star_contribution, time_slopes, precision=exact_reference))
    return jnp.stack(taylor_series)


def integrate(taylor_series, start_time, stop_time):
    quadrature_weights = jnp.array(taylor_weights(start_time, stop_time, taylor_series.shape[0]), jnp.float32)
    return jnp.einsum("h,hlui->lui", quadrature_weights, taylor_series, precision=exact_reference)


def face_values(field_state, projection):
    return jnp.einsum("bly,qyp->qlbp", projection, field_state, precision=exact_reference)


def advance(state_now, own_part, own_faces, beside, stiffness, projection, star_contribution, minus_part, coupling_part):
    incoming_flux = jnp.einsum("dvwe,wne->dvne", star_contribution, own_part, precision=exact_reference)
    volume_term = jnp.einsum("utx,uytz->yxz", stiffness, incoming_flux, precision=exact_reference)
    flux_terms = jnp.einsum("fvwe,wjfe->vjfe", minus_part, own_faces, precision=exact_reference)
    flux_terms = flux_terms + jnp.einsum("fvwe,wjfe->vjfe", coupling_part, beside, precision=exact_reference)
    surface_term = jnp.einsum("alz,qlad->qzd", projection, flux_terms, precision=exact_reference)
    return state_now + volume_term - surface_term


def to_blocks(array):
    split = array.reshape(array.shape[:-1] + (ELEMS // E_DEV, E_DEV))
    return jnp.moveaxis(split, -2, 0)


def from_blocks(array):
    joined = jnp.moveaxis(array, 0, -2)
    return joined.reshape(joined.shape[:-2] + (ELEMS,))


def reference(dofs, stiffness, projection, star, flux_minus, flux_plus, fault_flux, fault_faces, levels, face_source, send_source):
    device_count = ELEMS // E_DEV
    coupling = jnp.where(fault_faces[:, None, None, :] == 1, fault_flux[None, :, :, None], flux_plus)
    element_ids = jnp.arange(ELEMS, dtype=jnp.int32)
    device_ids = (element_ids // E_DEV)[None, :]
    local_column = device_ids * (4 * E_DEV) + face_source
    offset = face_source - 4 * E_DEV
    side_index = offset // (N_SUB * SEND)
    sub_index = (offset // SEND) % N_SUB
    slot_index = offset % SEND
    source_device = ((device_ids // N_SUB + side_index - 1) % N_DOM) * N_SUB + sub_index
    send_position = jnp.clip(source_device * SEND + slot_index, 0, device_count * SEND - 1).astype(jnp.int32)
    remote_column = source_device * (4 * E_DEV) + send_source[send_position]
    column = jnp.where(face_source < 4 * E_DEV, local_column, remote_column).astype(jnp.int32)
    column_order = to_blocks(column).reshape(-1)

    def beside_values(face_blocks):
        source_table = jnp.moveaxis(face_blocks, 0, 2).reshape(VARS * FACE_MODES, -1)
        picked = jnp.take(source_table, column_order, axis=1)
        return jnp.moveaxis(picked.reshape(VARS, FACE_MODES, device_count, 4, E_DEV), 2, 0)

    block_dofs = to_blocks(dofs)
    block_star = to_blocks(star)
    block_minus = to_blocks(flux_minus)
    block_coupling = to_blocks(coupling)
    block_fine = to_blocks(levels == 0)

    def phase_one(items):
        state_now, star_contribution = items
        taylor_series = derivatives(state_now, stiffness, star_contribution)
        first_half = integrate(taylor_series, 0.0, fine_step)
        second_half = integrate(taylor_series, fine_step, 2.0 * fine_step)
        return first_half, second_half, face_values(first_half, projection)

    first_b, second_b, first_faces_b = lax.map(phase_one, (block_dofs, block_star))
    beside_first_b = beside_values(first_faces_b)

    def phase_two(items):
        state_now, star_contribution, minus_part, coupling_part, is_fine, first_half, second_half, first_faces, beside_first = items
        updated = advance(state_now, first_half, first_faces, beside_first, stiffness, projection, star_contribution, minus_part, coupling_part)
        state_one = jnp.where(is_fine, updated, state_now)
        fine_integral = integrate(derivatives(state_one, stiffness, star_contribution), 0.0, fine_step)
        carried = jnp.where(is_fine, fine_integral, second_half)
        return state_one, carried, face_values(carried, projection)

    state_one_b, carried_b, carried_faces_b = lax.map(phase_two, (block_dofs, block_star, block_minus, block_coupling, block_fine, first_b, second_b, first_faces_b, beside_first_b))
    beside_carried_b = beside_values(carried_faces_b)

    def phase_three(items):
        state_now, star_contribution, minus_part, coupling_part, is_fine, first_half, second_half, beside_first, state_one, carried, carried_faces, beside_carried = items
        fine_new = advance(state_one, carried, carried_faces, beside_carried, stiffness, projection, star_contribution, minus_part, coupling_part)
        whole_step = first_half + second_half
        coarse_new = advance(state_now, whole_step, face_values(whole_step, projection), beside_first + beside_carried, stiffness, projection, star_contribution, minus_part, coupling_part)
        return jnp.where(is_fine, fine_new, coarse_new)

    result_b = lax.map(phase_three, (block_dofs, block_star, block_minus, block_coupling, block_fine, first_b, second_b, beside_first_b, state_one_b, carried_b, carried_faces_b, beside_carried_b))
    return from_blocks(result_b)
```

```python
import functools
import math

import jax
import jax.numpy as jnp
from jax import lax
from jax.experimental import pallas as pl
from jax.experimental.pallas import tpu as pltpu
from jax.sharding import PartitionSpec as P

MESH = pl.DeviceIdType.MESH
ORDER = 6
fine_step = 0.75
F32 = jnp.float32
BF16 = jnp.bfloat16


def taylor_weights(start_time, stop_time, term_count):
    return [
        (stop_time ** (term + 1) - start_time ** (term + 1)) / math.factorial(term + 1)
        for term in range(term_count)
    ]


def up_to(value, step):
    return -(-value // step) * step


def dot(a, b):
    return jnp.dot(a, b, preferred_element_type=F32)


def split(value):
    high = value.astype(BF16)
    return high, (value - high.astype(F32)).astype(BF16)


def stacked(value):
    return jnp.concatenate(split(value), axis=0)


def halves(product):
    rows = product.shape[0] // 2
    return product[:rows] + product[rows:]


def left_product(left_both, right):
    high, low = split(right)
    rows = left_both.shape[0] // 2
    return halves(dot(left_both, high)) + dot(left_both[:rows], low)


def right_product(left_both, right_high, right_low):
    rows = left_both.shape[0] // 2
    return halves(dot(left_both, right_high)) + dot(left_both[:rows], right_low)


def kernel(
    sizes,
    dofs,
    stiffness,
    projection,
    star,
    flux_minus,
    flux_plus,
    fault_flux,
    fault_faces,
    levels,
    face_source,
    send_source,
    out,
    rows_ref,
    ints,
    block_high,
    block_low,
    picks,
    flat,
    small,
    state,
    export,
    received,
    send_sem,
    recv_sem,
):
    n_dom, n_sub = sizes
    var_count, modes, elems = dofs.shape
    dims = stiffness.shape[0]
    faces, face_modes = projection.shape[0], projection.shape[1]
    slots = send_source.shape[1]
    lanes = var_count * elems
    m_pad = up_to(modes, 16)
    j_pad = up_to(face_modes, 16)
    j_sent = export.shape[1]
    per_table = elems // slots
    sources = 3 * n_sub
    tables = -(-sources // per_table)

    me_dom, me_sub = lax.axis_index("dom"), lax.axis_index("sub")
    partners = []
    for delta in (-1, 0, 1):
        for turn in range(n_sub):
            if delta or turn:
                partners.append(
                    (
                        (
                            lax.rem(me_dom + delta + n_dom, n_dom),
                            lax.rem(me_sub + turn, n_sub),
                        ),
                        (1 - delta) * n_sub + me_sub,
                    )
                )
    barrier = pltpu.get_barrier_semaphore()
    for target, _ in partners:
        pl.semaphore_signal(barrier, inc=1, device_id=target, device_id_type=MESH)

    state[...] = jnp.zeros_like(state)
    for v in range(var_count):
        state[0:modes, v * elems : (v + 1) * elems] = dofs[v]

    for d in range(dims):
        for v in range(var_count):
            rows_ref[d, 0:var_count, v * elems : (v + 1) * elems] = star[d, v]

    small[...] = jnp.zeros_like(small)
    for d in range(dims):
        small[0:modes, d * m_pad : d * m_pad + modes] = stiffness[d]
    forward = stacked(small[0:m_pad, 0 : dims * m_pad])

    mask = (
        lax.broadcasted_iota(jnp.int32, (elems, lanes), 1) % elems
        == lax.broadcasted_iota(jnp.int32, (elems, lanes), 0)
    )

    def spread(i):
        for w in range(var_count):
            row = rows_ref[i, w : w + 1, :]
            high = row.astype(BF16).astype(F32)
            low = row - high
            at = slice(w * elems, (w + 1) * elems)
            block_high[i, at, :] = jnp.where(mask, high, 0.0).astype(BF16)
            block_low[i, at, :] = jnp.where(mask, low, 0.0).astype(BF16)

    for d in range(dims):
        spread(d)

    def turned(value):
        both = stacked(value)
        return [
            right_product(both, block_high[d], block_low[d]) for d in range(dims)
        ]

    def series(value, weight_sets):
        totals = [weights[0] * value for weights in weight_sets]
        for term in range(1, ORDER):
            value = left_product(forward, jnp.concatenate(turned(value), axis=0))
            totals = [
                total + weights[term] * value
                for total, weights in zip(totals, weight_sets)
            ]
        return totals

    first_weights = taylor_weights(0.0, fine_step, ORDER)
    second_weights = taylor_weights(fine_step, 2.0 * fine_step, ORDER)
    first_half, second_half = series(state[...], (first_weights, second_weights))

    flat[...] = jnp.zeros_like(flat)
    for d in range(dims):
        flat[d * m_pad : d * m_pad + modes, 0:modes] = stiffness[d]
    base = dims * m_pad
    for f in range(faces):
        flat[base + f * j_pad : base + f * j_pad + face_modes, 0:modes] = -projection[f]
    base_fault = base + faces * j_pad
    flat[base_fault : base_fault + var_count, 0:var_count] = fault_flux[...]
    project = stacked(-flat[base : base + faces * j_pad, 0:m_pad])
    flipped = jnp.transpose(flat[...])
    back = stacked(flipped[0:m_pad, 0:base_fault])

    for i in range(per_table):
        ints[9:10, i * slots : (i + 1) * slots] = send_source[...]
    send_row = ints[9:10, 0:elems]
    for v in range(var_count):
        at = slice(v * elems, (v + 1) * elems)
        ints[0:faces, at] = face_source[...]
        ints[4 : 4 + faces, at] = fault_faces[...]
        ints[8:9, at] = levels[...]
        ints[9:10, at] = send_row

    row_id = lax.broadcasted_iota(jnp.int32, (lanes, lanes), 0)
    lane_id = lax.broadcasted_iota(jnp.int32, (lanes, lanes), 1)
    key = jnp.where(row_id // elems == lane_id // elems, row_id % elems, -(2**20))

    def pick(row, f):
        return jnp.where(key == ints[row : row + 1, :] - f * elems, 1.0, 0.0).astype(BF16)

    def face_halves(value):
        both = stacked(left_product(project, value))
        count = faces * j_pad
        return [
            jnp.concatenate(
                [
                    both[f * j_pad : (f + 1) * j_pad],
                    both[count + f * j_pad : count + (f + 1) * j_pad],
                ],
                axis=0,
            )
            for f in range(faces)
        ]

    def total_of(parts):
        return functools.reduce(lambda a, b: a + b, parts)

    send_picks = [pick(9, f) for f in range(faces)]
    own_slot = n_sub + me_sub

    def launch(phase, face_parts):
        block = halves(
            total_of([dot(part, one) for part, one in zip(face_parts, send_picks)])
        )[0:j_sent]
        export[phase] = block
        copies = []
        for i, (target, slot) in enumerate(partners):
            copy = pltpu.make_async_remote_copy(
                src_ref=export.at[phase],
                dst_ref=received.at[phase, slot],
                send_sem=send_sem.at[phase, i],
                recv_sem=recv_sem.at[phase, i],
                device_id=target,
                device_id_type=MESH,
            )
            copy.start()
            copies.append(copy)
        received[phase, own_slot] = block
        return copies

    def local_part(value, face_parts):
        volume = turned(value)
        own = [
            right_product(face_parts[f], block_high[dims + f], block_low[dims + f])
            for f in range(faces)
        ]
        beside = [
            total_of([dot(face_parts[g], picks[g, f]) for g in range(faces)])
            for f in range(faces)
        ]
        return volume, own, beside

    table_lane = lax.broadcasted_iota(jnp.int32, (j_sent, lanes), 1) % elems // slots

    def finish(phase, copies, parts):
        volume, own, beside = parts
        for copy in copies:
            copy.wait()
        table_parts = []
        for t in range(tables):
            table = jnp.zeros((j_sent, lanes), F32)
            for i in range(min(per_table, sources - t * per_table)):
                table = jnp.where(
                    table_lane == i, received[phase, t * per_table + i], table
                )
            if j_pad > j_sent:
                table = jnp.concatenate(
                    [table, jnp.zeros((j_pad - j_sent, lanes), F32)], axis=0
                )
            table_parts.append(stacked(table))
        flux = []
        for f in range(faces):
            gathered = halves(
                beside[f]
                + total_of(
                    [dot(table_parts[t], picks[faces + t, f]) for t in range(tables)]
                )
            )
            at = dims + faces + f
            flux.append(
                own[f] + right_product(stacked(gathered), block_high[at], block_low[at])
            )
        return left_product(back, jnp.concatenate(volume + flux, axis=0))

    face_parts = face_halves(first_half)
    pl.semaphore_wait(barrier, len(partners))
    copies = launch(0, face_parts)

    for v in range(var_count):
        at = slice(v * elems, (v + 1) * elems)
        fault_column = flipped[0:var_count, base_fault + v : base_fault + v + 1]
        for f in range(faces):
            rows_ref[dims + f, 0:var_count, at] = flux_minus[f, v]
            rows_ref[dims + faces + f, 0:var_count, at] = jnp.where(
                fault_faces[f : f + 1, :] == 1, fault_column, flux_plus[f, v]
            )
    for i in range(dims, dims + 2 * faces):
        spread(i)
    for f in range(faces):
        for g in range(faces + tables):
            picks[g, f] = pick(f, g)

    parts = local_part(first_half, face_parts)
    moved = state[...] + finish(0, copies, parts)
    (fine_half,) = series(moved, (first_weights,))
    carried = jnp.where(ints[8:9, :] == 0, fine_half, second_half)
    face_parts = face_halves(carried)
    copies = launch(1, face_parts)
    parts = local_part(carried, face_parts)
    result = moved + finish(1, copies, parts)
    for v in range(var_count):
        out[v] = result[0:modes, v * elems : (v + 1) * elems]


def solution(mesh):
    n_dom, n_sub = mesh.shape["dom"], mesh.shape["sub"]

    def per_device(
        dofs,
        stiffness,
        projection,
        star,
        flux_minus,
        flux_plus,
        fault_flux,
        fault_faces,
        levels,
        face_source,
        send_source,
    ):
        var_count, modes, elems = dofs.shape
        dims = stiffness.shape[0]
        faces, face_modes = projection.shape[0], projection.shape[1]
        slots = send_source.shape[0]
        lanes = var_count * elems
        m_pad, j_pad = up_to(modes, 16), up_to(face_modes, 16)
        j_sent = up_to(face_modes, 8)
        sources = 3 * n_sub
        tables = -(-sources // (elems // slots))
        blocks = dims + 2 * faces
        flat_rows = up_to(dims * m_pad + faces * j_pad + var_count, 128)
        vmem = pl.BlockSpec(memory_space=pltpu.VMEM)
        return pl.pallas_call(
            functools.partial(kernel, (n_dom, n_sub)),
            out_shape=jax.ShapeDtypeStruct(dofs.shape, F32),
            in_specs=[vmem] * 11,
            out_specs=vmem,
            scratch_shapes=[
                pltpu.VMEM((blocks, up_to(var_count, 8), lanes), F32),
                pltpu.VMEM((16, lanes), jnp.int32),
                pltpu.VMEM((blocks, lanes, lanes), BF16),
                pltpu.VMEM((blocks, lanes, lanes), BF16),
                pltpu.VMEM((faces + tables, faces, lanes, lanes), BF16),
                pltpu.VMEM((flat_rows, 128), F32),
                pltpu.VMEM((m_pad, up_to(dims * m_pad, 128)), F32),
                pltpu.VMEM((m_pad, lanes), F32),
                pltpu.VMEM((2, j_sent, lanes), F32),
                pltpu.VMEM((2, sources, j_sent, lanes), F32),
                pltpu.SemaphoreType.DMA((2, sources - 1)),
                pltpu.SemaphoreType.DMA((2, sources - 1)),
            ],
            compiler_params=pltpu.CompilerParams(
                collective_id=0,
                has_side_effects=True,
                vmem_limit_bytes=48 * 1024 * 1024,
            ),
            name="window",
        )(
            dofs,
            stiffness,
            projection,
            star,
            flux_minus,
            flux_plus,
            fault_flux,
            fault_faces,
            levels.reshape(1, -1),
            face_source,
            send_source.reshape(1, -1),
        )

    return jax.shard_map(
        per_device,
        mesh=mesh,
        in_specs=(
            P(None, None, ("dom", "sub")),
            P(),
            P(),
            P(None, None, None, ("dom", "sub")),
            P(None, None, None, ("dom", "sub")),
            P(None, None, None, ("dom", "sub")),
            P(),
            P(None, ("dom", "sub")),
            P(("dom", "sub")),
            P(None, ("dom", "sub")),
            P(("dom", "sub")),
        ),
        out_specs=P(None, None, ("dom", "sub")),
        check_vma=False,
    )
```

```python
import functools
import math

import jax
import jax.numpy as jnp
from jax import lax
from jax.experimental import pallas as pl
from jax.experimental.pallas import tpu as pltpu
from jax.sharding import PartitionSpec as P

MESH = pl.DeviceIdType.MESH
ORDER = 6
fine_step = 0.75
F32 = jnp.float32
BF16 = jnp.bfloat16


def taylor_weights(start_time, stop_time, term_count):
    return [
        (stop_time ** (term + 1) - start_time ** (term + 1)) / math.factorial(term + 1)
        for term in range(term_count)
    ]


def up_to(value, step):
    return -(-value // step) * step


def dot(a, b):
    return jnp.dot(a, b, preferred_element_type=F32)


def split(value):
    high = value.astype(BF16)
    return high, (value - high.astype(F32)).astype(BF16)


def stacked(value):
    return jnp.concatenate(split(value), axis=0)


def halves(product):
    rows = product.shape[0] // 2
    return product[:rows] + product[rows:]


def left_product(left_both, right):
    high, low = split(right)
    rows = left_both.shape[0] // 2
    return halves(dot(left_both, high)) + dot(left_both[:rows], low)


def right_product(left_both, right_high, right_low):
    rows = left_both.shape[0] // 2
    return halves(dot(left_both, right_high)) + dot(left_both[:rows], right_low)


def kernel(
    sizes,
    dofs_hbm,
    stiffness_hbm,
    projection_hbm,
    star_hbm,
    minus_hbm,
    plus_hbm,
    fault_hbm,
    fault_faces,
    levels,
    face_source,
    send_source,
    out,
    dofs,
    stiffness,
    projection,
    star,
    flux_minus,
    flux_plus,
    fault_flux,
    star_rows,
    minus_rows,
    plus_rows,
    fault_rows,
    ints,
    block_high,
    block_low,
    picks,
    send_picks,
    remote_picks,
    flat,
    small,
    turn_ref,
    export,
    received,
    table_ref,
    load_sem,
    send_sem,
    recv_sem,
):
    n_dom, n_sub = sizes
    var_count, elems, modes = dofs.shape
    dims = stiffness.shape[0]
    face_modes, faces = projection.shape[0], projection.shape[1]
    slots = send_source.shape[1]
    lanes = var_count * elems
    m_pad = up_to(modes, 16)
    j_pad = up_to(face_modes, 16)
    groups = up_to(face_modes, 8) // 8
    width = var_count * slots
    sources = 3 * n_sub
    tables, _, table_lanes = table_ref.shape
    per_table = table_lanes // width

    loads = [
        pltpu.make_async_copy(src, dst, load_sem.at[i])
        for i, (src, dst) in enumerate(
            (
                (star_hbm, star),
                (dofs_hbm, dofs),
                (stiffness_hbm, stiffness),
                (projection_hbm, projection),
                (fault_hbm, fault_flux),
                (minus_hbm, flux_minus),
                (plus_hbm, flux_plus),
            )
        )
    ]
    for load in loads:
        load.start()

    me_dom, me_sub = lax.axis_index("dom"), lax.axis_index("sub")
    partners = []
    for delta in (-1, 0, 1):
        for turn in range(n_sub):
            if delta or turn:
                partners.append(
                    (
                        (
                            lax.rem(me_dom + delta + n_dom, n_dom),
                            lax.rem(me_sub + turn, n_sub),
                        ),
                        (1 - delta) * n_sub + me_sub,
                    )
                )
    barrier = pltpu.get_barrier_semaphore()
    for target, _ in partners:
        pl.semaphore_signal(barrier, inc=1, device_id=target, device_id_type=MESH)

    small[...] = jnp.zeros_like(small)
    flat[...] = jnp.zeros_like(flat)
    turn_ref[...] = jnp.zeros_like(turn_ref)
    table_ref[...] = jnp.zeros_like(table_ref)
    export[...] = jnp.zeros_like(export)

    mask = (
        lax.broadcasted_iota(jnp.int32, (elems, lanes), 1) % elems
        == lax.broadcasted_iota(jnp.int32, (elems, lanes), 0)
    )

    def spread(rows, f, i):
        for w in range(var_count):
            row = rows[w, f : f + 1, :]
            high = row.astype(BF16).astype(F32)
            low = row - high
            at = slice(w * elems, (w + 1) * elems)
            block_high[i, at, :] = jnp.where(mask, high, 0.0).astype(BF16)
            block_low[i, at, :] = jnp.where(mask, low, 0.0).astype(BF16)

    loads[0].wait()
    for v in range(var_count):
        star_rows[:, :, v * elems : (v + 1) * elems] = star[v]
    for d in range(dims):
        spread(star_rows, d, d)

    loads[1].wait()
    turn_ref[0:lanes, 0:modes] = dofs[...].reshape(lanes, modes)
    state = jnp.transpose(turn_ref[...])[0:m_pad, 0:lanes]

    loads[2].wait()
    for d in range(dims):
        small[0:modes, d * m_pad : d * m_pad + modes] = stiffness[d]
    forward = stacked(small[0:m_pad, 0 : dims * m_pad])

    def turned(value):
        both = stacked(value)
        return [
            right_product(both, block_high[d], block_low[d]) for d in range(dims)
        ]

    def series(value, weight_sets):
        totals = [weights[0] * value for weights in weight_sets]
        for term in range(1, ORDER):
            value = left_product(forward, jnp.concatenate(turned(value), axis=0))
            totals = [
                total + weights[term] * value
                for total, weights in zip(totals, weight_sets)
            ]
        return totals

    first_weights = taylor_weights(0.0, fine_step, ORDER)
    second_weights = taylor_weights(fine_step, 2.0 * fine_step, ORDER)

    loads[3].wait()
    loads[4].wait()
    for d in range(dims):
        flat[d * m_pad : d * m_pad + modes, 0:modes] = stiffness[d]
    base = dims * m_pad
    for f in range(faces):
        flat[base + f * j_pad : base + f * j_pad + face_modes, 0:modes] = -projection[
            :, f, :
        ]
    base_fault = base + faces * j_pad
    flat[base_fault : base_fault + var_count, 0:var_count] = fault_flux[...]

    send_row = send_source[...]
    for i in range(width // slots):
        ints[9:10, i * slots : (i + 1) * slots] = send_row
    for v in range(var_count):
        at = slice(v * elems, (v + 1) * elems)
        ints[0:faces, at] = face_source[...]
        ints[4 : 4 + faces, at] = fault_faces[...]
        ints[8:9, at] = levels[...]

    def code(shape, dim, element_count):
        index = lax.broadcasted_iota(jnp.int32, shape, dim)
        return index // element_count, index % element_count

    row_var, row_elem = code((lanes, width), 0, elems)
    lane_var, _ = code((lanes, width), 1, slots)
    send_key = jnp.where(row_var == lane_var, row_elem, -(2**20))
    for f in range(faces):
        send_picks[f] = jnp.where(
            send_key == ints[9:10, 0:width] - f * elems, 1.0, 0.0
        ).astype(BF16)

    first_half, second_half = series(state, (first_weights, second_weights))

    project = stacked(-flat[base : base + faces * j_pad, 0:m_pad])
    flipped = jnp.transpose(flat[...])
    back = stacked(flipped[0:m_pad, 0:base_fault])

    def face_halves(value):
        both = stacked(left_product(project, value))
        count = faces * j_pad
        return [
            jnp.concatenate(
                [
                    both[f * j_pad : (f + 1) * j_pad],
                    both[count + f * j_pad : count + (f + 1) * j_pad],
                ],
                axis=0,
            )
            for f in range(faces)
        ]

    def total_of(parts):
        return functools.reduce(lambda a, b: a + b, parts)

    own_slot = n_sub + me_sub

    def launch(phase, face_parts):
        block = halves(
            total_of([dot(face_parts[f], send_picks[f]) for f in range(faces)])
        )
        for g in range(groups):
            export[phase, :, g * width : (g + 1) * width] = block[8 * g : 8 * g + 8]
        copies = []
        for i, (target, slot) in enumerate(partners):
            copy = pltpu.make_async_remote_copy(
                src_ref=export.at[phase],
                dst_ref=received.at[phase, slot],
                send_sem=send_sem.at[phase, i],
                recv_sem=recv_sem.at[phase, i],
                device_id=target,
                device_id_type=MESH,
            )
            copy.start()
            copies.append(copy)
        received[phase, own_slot] = export[phase]
        return copies

    def local_part(value, face_parts):
        volume = turned(value)
        own = [
            right_product(face_parts[f], block_high[dims + f], block_low[dims + f])
            for f in range(faces)
        ]
        beside = [
            total_of([dot(face_parts[g], picks[g, f]) for g in range(faces)])
            for f in range(faces)
        ]
        return volume, own, beside

    def finish(phase, copies, parts):
        volume, own, beside = parts
        for copy in copies:
            copy.wait()
        for k in range(sources):
            t, at = k // per_table, k % per_table * width
            for g in range(groups):
                table_ref[t, 8 * g : 8 * g + 8, at : at + width] = received[
                    phase, k, :, g * width : (g + 1) * width
                ]
        table_parts = [stacked(table_ref[t]) for t in range(tables)]
        flux = []
        for f in range(faces):
            gathered = halves(
                beside[f]
                + total_of([dot(table_parts[t], remote_picks[t, f]) for t in range(tables)])
            )
            at = dims + faces + f
            flux.append(
                own[f] + right_product(stacked(gathered), block_high[at], block_low[at])
            )
        return left_product(back, jnp.concatenate(volume + flux, axis=0))

    face_parts = face_halves(first_half)
    pl.semaphore_wait(barrier, len(partners))
    copies = launch(0, face_parts)

    loads[5].wait()
    loads[6].wait()
    for v in range(var_count):
        at = slice(v * elems, (v + 1) * elems)
        minus_rows[:, :, at] = flux_minus[v]
        plus_rows[:, :, at] = flux_plus[v]
        fault_rows[0:var_count, at] = jnp.broadcast_to(
            flipped[0:var_count, base_fault + v : base_fault + v + 1], (var_count, elems)
        )
    on_fault = ints[4 : 4 + faces, :] == 1
    for w in range(var_count):
        plus_rows[w] = jnp.where(on_fault, fault_rows[w : w + 1, :], plus_rows[w])
    for f in range(faces):
        spread(minus_rows, f, dims + f)
        spread(plus_rows, f, dims + faces + f)
    row_var, row_elem = code((lanes, lanes), 0, elems)
    lane_var, _ = code((lanes, lanes), 1, elems)
    key = jnp.where(row_var == lane_var, row_elem, -(2**20))
    source_id, inside = code((table_lanes, lanes), 0, width)
    slot_var, slot = inside // slots, inside % slots
    lane_var, _ = code((table_lanes, lanes), 1, elems)
    remote_key = jnp.where(
        slot_var == lane_var, faces * elems + source_id * slots + slot, -(2**20)
    )
    for f in range(faces):
        wanted = ints[f : f + 1, :]
        for g in range(faces):
            picks[g, f] = jnp.where(key == wanted - g * elems, 1.0, 0.0).astype(BF16)
        for t in range(tables):
            remote_picks[t, f] = jnp.where(
                remote_key == wanted - t * per_table * slots, 1.0, 0.0
            ).astype(BF16)

    parts = local_part(first_half, face_parts)
    moved = state + finish(0, copies, parts)
    (fine_half,) = series(moved, (first_weights,))
    carried = jnp.where(ints[8:9, :] == 0, fine_half, second_half)
    face_parts = face_halves(carried)
    copies = launch(1, face_parts)
    parts = local_part(carried, face_parts)
    result = moved + finish(1, copies, parts)
    turned_back = jnp.transpose(
        jnp.concatenate(
            [
                jnp.concatenate(
                    [result, jnp.zeros((m_pad, turn_ref.shape[0] - lanes), F32)], axis=1
                ),
                jnp.zeros((128 - m_pad, turn_ref.shape[0]), F32),
            ],
            axis=0,
        )
    )
    out[...] = turned_back[0:lanes, 0:modes].reshape(var_count, elems, modes)


def solution(mesh):
    n_dom, n_sub = mesh.shape["dom"], mesh.shape["sub"]

    def per_device(
        dofs,
        stiffness,
        projection,
        star,
        flux_minus,
        flux_plus,
        fault_flux,
        fault_faces,
        levels,
        face_source,
        send_source,
    ):
        var_count, modes, elems = dofs.shape
        dims = stiffness.shape[0]
        faces, face_modes = projection.shape[0], projection.shape[1]
        slots = send_source.shape[0]
        lanes = var_count * elems
        m_pad, j_pad = up_to(modes, 16), up_to(face_modes, 16)
        width = var_count * slots
        sources = 3 * n_sub
        tables = -(-sources // (256 // width))
        per_table = -(-sources // tables)
        blocks = dims + 2 * faces
        flat_rows = up_to(dims * m_pad + faces * j_pad + var_count, 128)
        vmem = pl.BlockSpec(memory_space=pltpu.VMEM)
        whole = pl.BlockSpec(memory_space=pltpu.HBM)
        moved = [
            jnp.transpose(dofs, (0, 2, 1)),
            stiffness,
            jnp.transpose(projection, (1, 0, 2)),
            jnp.transpose(star, (1, 2, 0, 3)),
            jnp.transpose(flux_minus, (1, 2, 0, 3)),
            jnp.transpose(flux_plus, (1, 2, 0, 3)),
            fault_flux,
        ]
        result = pl.pallas_call(
            functools.partial(kernel, (n_dom, n_sub)),
            out_shape=jax.ShapeDtypeStruct((var_count, elems, modes), F32),
            in_specs=[whole] * 7 + [vmem] * 4,
            out_specs=vmem,
            scratch_shapes=[pltpu.VMEM(one.shape, F32) for one in moved]
            + [
                pltpu.VMEM((var_count, dims, lanes), F32),
                pltpu.VMEM((var_count, faces, lanes), F32),
                pltpu.VMEM((var_count, faces, lanes), F32),
                pltpu.VMEM((up_to(var_count, 8), lanes), F32),
                pltpu.VMEM((16, lanes), jnp.int32),
                pltpu.VMEM((blocks, lanes, lanes), BF16),
                pltpu.VMEM((blocks, lanes, lanes), BF16),
                pltpu.VMEM((faces, faces, lanes, lanes), BF16),
                pltpu.VMEM((faces, lanes, width), BF16),
                pltpu.VMEM((tables, faces, per_table * width, lanes), BF16),
                pltpu.VMEM((flat_rows, 128), F32),
                pltpu.VMEM((m_pad, up_to(dims * m_pad, 128)), F32),
                pltpu.VMEM((up_to(lanes, 128), 128), F32),
                pltpu.VMEM((2, 8, 128), F32),
                pltpu.VMEM((2, sources, 8, 128), F32),
                pltpu.VMEM((tables, j_pad, per_table * width), F32),
                pltpu.SemaphoreType.DMA((len(moved),)),
                pltpu.SemaphoreType.DMA((2, sources - 1)),
                pltpu.SemaphoreType.DMA((2, sources - 1)),
            ],
            compiler_params=pltpu.CompilerParams(
                collective_id=0,
                has_side_effects=True,
                vmem_limit_bytes=48 * 1024 * 1024,
            ),
            name="window",
        )(
            *moved,
            fault_faces,
            levels.reshape(1, -1),
            face_source,
            send_source.reshape(1, -1),
        )
        return jnp.transpose(result, (0, 2, 1))

    return jax.shard_map(
        per_device,
        mesh=mesh,
        in_specs=(
            P(None, None, ("dom", "sub")),
            P(),
            P(),
            P(None, None, None, ("dom", "sub")),
            P(None, None, None, ("dom", "sub")),
            P(None, None, None, ("dom", "sub")),
            P(),
            P(None, ("dom", "sub")),
            P(("dom", "sub")),
            P(None, ("dom", "sub")),
            P(("dom", "sub")),
        ),
        out_specs=P(None, None, ("dom", "sub")),
        check_vma=False,
    )
```

```python
import functools
import math

import jax
import jax.numpy as jnp
from jax import lax
from jax.experimental import pallas as pl
from jax.experimental.pallas import tpu as pltpu
from jax.sharding import PartitionSpec as P

MESH = pl.DeviceIdType.MESH
ORDER = 6
fine_step = 0.75
F32 = jnp.float32
BF16 = jnp.bfloat16


def taylor_weights(start_time, stop_time, term_count):
    return [
        (stop_time ** (term + 1) - start_time ** (term + 1)) / math.factorial(term + 1)
        for term in range(term_count)
    ]


def up_to(value, step):
    return -(-value // step) * step


def dot(a, b):
    return jnp.dot(a, b, preferred_element_type=F32)


def split(value):
    high = value.astype(BF16)
    return high, (value - high.astype(F32)).astype(BF16)


def stacked(value):
    return jnp.concatenate(split(value), axis=0)


def halves(product):
    rows = product.shape[0] // 2
    return product[:rows] + product[rows:]


def left_product(left_both, right):
    high, low = split(right)
    rows = left_both.shape[0] // 2
    return halves(dot(left_both, high)) + dot(left_both[:rows], low)


def right_product(left_both, right_high, right_low):
    rows = left_both.shape[0] // 2
    return halves(dot(left_both, right_high)) + dot(left_both[:rows], right_low)


def kernel(
    sizes,
    dofs_hbm,
    stiffness_hbm,
    projection_hbm,
    star_hbm,
    minus_hbm,
    plus_hbm,
    fault_hbm,
    fault_faces,
    levels,
    face_source,
    send_source,
    out,
    dofs,
    stiffness,
    projection,
    star,
    flux_minus,
    flux_plus,
    fault_flux,
    star_rows,
    minus_rows,
    plus_rows,
    fault_rows,
    ints,
    block_high,
    block_low,
    picks,
    send_picks,
    remote_picks,
    flat,
    small,
    turn_ref,
    export,
    received,
    table_ref,
    load_sem,
    send_sem,
    recv_sem,
):
    n_dom, n_sub = sizes
    var_count, elems, modes = dofs.shape
    dims = stiffness.shape[0]
    face_modes, faces = projection.shape[0], projection.shape[1]
    slots = send_source.shape[1]
    lanes = var_count * elems
    m_pad = up_to(modes, 16)
    j_pad = up_to(face_modes, 16)
    groups = up_to(face_modes, 8) // 8
    width = var_count * slots
    sources = 3 * n_sub
    tables, _, table_lanes = table_ref.shape
    per_table = table_lanes // width

    loads = [
        pltpu.make_async_copy(src, dst, load_sem.at[i])
        for i, (src, dst) in enumerate(
            (
                (star_hbm, star),
                (dofs_hbm, dofs),
                (stiffness_hbm, stiffness),
                (projection_hbm, projection),
                (fault_hbm, fault_flux),
                (minus_hbm, flux_minus),
                (plus_hbm, flux_plus),
            )
        )
    ]
    for load in loads:
        load.start()

    me_dom, me_sub = lax.axis_index("dom"), lax.axis_index("sub")
    partners = []
    for delta in (-1, 0, 1):
        for turn in range(n_sub):
            if delta or turn:
                partners.append(
                    (
                        (
                            lax.rem(me_dom + delta + n_dom, n_dom),
                            lax.rem(me_sub + turn, n_sub),
                        ),
                        (1 - delta) * n_sub + me_sub,
                    )
                )
    barrier = pltpu.get_barrier_semaphore()
    for target, _ in partners:
        pl.semaphore_signal(barrier, inc=1, device_id=target, device_id_type=MESH)

    small[...] = jnp.zeros_like(small)
    flat[...] = jnp.zeros_like(flat)
    turn_ref[...] = jnp.zeros_like(turn_ref)
    table_ref[...] = jnp.zeros_like(table_ref)
    export[...] = jnp.zeros_like(export)

    mask = (
        lax.broadcasted_iota(jnp.int32, (elems, lanes), 1) % elems
        == lax.broadcasted_iota(jnp.int32, (elems, lanes), 0)
    )

    def spread(rows, f, i):
        for w in range(var_count):
            row = rows[w, f : f + 1, :]
            high = row.astype(BF16).astype(F32)
            low = row - high
            at = slice(w * elems, (w + 1) * elems)
            block_high[i, at, :] = jnp.where(mask, high, 0.0).astype(BF16)
            block_low[i, at, :] = jnp.where(mask, low, 0.0).astype(BF16)

    loads[0].wait()
    for v in range(var_count):
        star_rows[:, :, v * elems : (v + 1) * elems] = star[v]
    for d in range(dims):
        spread(star_rows, d, d)

    loads[1].wait()
    turn_ref[0:lanes, 0:modes] = dofs[...].reshape(lanes, modes)
    state = jnp.transpose(turn_ref[...])[0:m_pad, 0:lanes]

    loads[2].wait()
    for d in range(dims):
        small[0:modes, d * m_pad : d * m_pad + modes] = stiffness[d]
    forward = stacked(small[0:m_pad, 0 : dims * m_pad])

    def turned(value):
        both = stacked(value)
        return [
            right_product(both, block_high[d], block_low[d]) for d in range(dims)
        ]

    def series(value, weight_sets):
        totals = [weights[0] * value for weights in weight_sets]
        for term in range(1, ORDER):
            value = left_product(forward, jnp.concatenate(turned(value), axis=0))
            totals = [
                total + weights[term] * value
                for total, weights in zip(totals, weight_sets)
            ]
        return totals

    first_weights = taylor_weights(0.0, fine_step, ORDER)
    second_weights = taylor_weights(fine_step, 2.0 * fine_step, ORDER)

    loads[3].wait()
    loads[4].wait()
    for d in range(dims):
        flat[d * m_pad : d * m_pad + modes, 0:modes] = stiffness[d]
    base = dims * m_pad
    for f in range(faces):
        flat[base + f * j_pad : base + f * j_pad + face_modes, 0:modes] = -projection[
            :, f, :
        ]
    base_fault = base + faces * j_pad
    flat[base_fault : base_fault + var_count, 0:var_count] = fault_flux[...]

    send_row = send_source[...]
    for i in range(width // slots):
        ints[9:10, i * slots : (i + 1) * slots] = send_row
    for v in range(var_count):
        at = slice(v * elems, (v + 1) * elems)
        ints[0:faces, at] = face_source[...]
        ints[4 : 4 + faces, at] = fault_faces[...]
        ints[8:9, at] = levels[...]

    def code(shape, dim, element_count):
        index = lax.broadcasted_iota(jnp.int32, shape, dim)
        return index // element_count, index % element_count

    row_var, row_elem = code((lanes, width), 0, elems)
    lane_var, _ = code((lanes, width), 1, slots)
    send_key = jnp.where(row_var == lane_var, row_elem, -(2**20))
    for f in range(faces):
        send_picks[f] = jnp.where(
            send_key == ints[9:10, 0:width] - f * elems, 1.0, 0.0
        ).astype(BF16)

    first_half, second_half = series(state, (first_weights, second_weights))

    project = stacked(-flat[base : base + faces * j_pad, 0:m_pad])
    flipped = jnp.transpose(flat[...])
    back = stacked(flipped[0:m_pad, 0:base_fault])

    def face_halves(value):
        both = stacked(left_product(project, value))
        count = faces * j_pad
        return [
            jnp.concatenate(
                [
                    both[f * j_pad : (f + 1) * j_pad],
                    both[count + f * j_pad : count + (f + 1) * j_pad],
                ],
                axis=0,
            )
            for f in range(faces)
        ]

    def total_of(parts):
        return functools.reduce(lambda a, b: a + b, parts)

    own_slot = n_sub + me_sub

    def launch(phase, face_parts):
        block = halves(
            total_of([dot(face_parts[f], send_picks[f]) for f in range(faces)])
        )
        for g in range(groups):
            export[phase, :, g * width : (g + 1) * width] = block[8 * g : 8 * g + 8]
        copies = []
        for i, (target, slot) in enumerate(partners):
            copy = pltpu.make_async_remote_copy(
                src_ref=export.at[phase],
                dst_ref=received.at[phase, slot],
                send_sem=send_sem.at[phase, i],
                recv_sem=recv_sem.at[phase, i],
                device_id=target,
                device_id_type=MESH,
            )
            copy.start()
            copies.append(copy)
        received[phase, own_slot] = export[phase]
        return copies

    def local_part(value, face_parts):
        volume = turned(value)
        own = [
            right_product(face_parts[f], block_high[dims + f], block_low[dims + f])
            for f in range(faces)
        ]
        beside = [
            total_of([dot(face_parts[g], picks[g, f]) for g in range(faces)])
            for f in range(faces)
        ]
        return volume, own, beside

    def finish(phase, copies, parts):
        volume, own, beside = parts
        for copy in copies:
            copy.wait()
        for k in range(sources):
            t, at = k // per_table, k % per_table * width
            for g in range(groups):
                table_ref[t, 8 * g : 8 * g + 8, at : at + width] = received[
                    phase, k, :, g * width : (g + 1) * width
                ]
        table_parts = [stacked(table_ref[t]) for t in range(tables)]
        flux = []
        for f in range(faces):
            gathered = halves(
                beside[f]
                + total_of([dot(table_parts[t], remote_picks[t, f]) for t in range(tables)])
            )
            at = dims + faces + f
            flux.append(
                own[f] + right_product(stacked(gathered), block_high[at], block_low[at])
            )
        return left_product(back, jnp.concatenate(volume + flux, axis=0))

    face_parts = face_halves(first_half)
    pl.semaphore_wait(barrier, len(partners))
    copies = launch(0, face_parts)

    loads[5].wait()
    loads[6].wait()
    for v in range(var_count):
        at = slice(v * elems, (v + 1) * elems)
        minus_rows[:, :, at] = flux_minus[v]
        plus_rows[:, :, at] = flux_plus[v]
        fault_rows[0:var_count, at] = jnp.broadcast_to(
            flipped[0:var_count, base_fault + v : base_fault + v + 1], (var_count, elems)
        )
    on_fault = ints[4 : 4 + faces, :] == 1
    for w in range(var_count):
        plus_rows[w] = jnp.where(on_fault, fault_rows[w : w + 1, :], plus_rows[w])
    for f in range(faces):
        spread(minus_rows, f, dims + f)
        spread(plus_rows, f, dims + faces + f)
    row_var, row_elem = code((lanes, lanes), 0, elems)
    lane_var, _ = code((lanes, lanes), 1, elems)
    key = jnp.where(row_var == lane_var, row_elem, -(2**20))
    source_id, inside = code((table_lanes, lanes), 0, width)
    slot_var, slot = inside // slots, inside % slots
    lane_var, _ = code((table_lanes, lanes), 1, elems)
    remote_key = jnp.where(
        slot_var == lane_var, faces * elems + source_id * slots + slot, -(2**20)
    )
    for f in range(faces):
        wanted = ints[f : f + 1, :]
        for g in range(faces):
            picks[g, f] = jnp.where(key == wanted - g * elems, 1.0, 0.0).astype(BF16)
        for t in range(tables):
            remote_picks[t, f] = jnp.where(
                remote_key == wanted - t * per_table * slots, 1.0, 0.0
            ).astype(BF16)

    parts = local_part(first_half, face_parts)
    moved = state + finish(0, copies, parts)
    (fine_half,) = series(moved, (first_weights,))
    carried = jnp.where(ints[8:9, :] == 0, fine_half, second_half)
    face_parts = face_halves(carried)
    copies = launch(1, face_parts)
    parts = local_part(carried, face_parts)
    result = moved + finish(1, copies, parts)
    turned_back = jnp.transpose(
        jnp.concatenate(
            [
                jnp.concatenate(
                    [result, jnp.zeros((m_pad, turn_ref.shape[0] - lanes), F32)], axis=1
                ),
                jnp.zeros((128 - m_pad, turn_ref.shape[0]), F32),
            ],
            axis=0,
        )
    )
    out[...] = turned_back[0:lanes, 0:modes].reshape(var_count, elems, modes)


def solution(mesh):
    n_dom, n_sub = mesh.shape["dom"], mesh.shape["sub"]

    def per_device(
        dofs,
        stiffness,
        projection,
        star,
        flux_minus,
        flux_plus,
        fault_flux,
        fault_faces,
        levels,
        face_source,
        send_source,
    ):
        var_count, modes, elems = dofs.shape
        dims = stiffness.shape[0]
        faces, face_modes = projection.shape[0], projection.shape[1]
        slots = send_source.shape[0]
        lanes = var_count * elems
        m_pad, j_pad = up_to(modes, 16), up_to(face_modes, 16)
        width = var_count * slots
        sources = 3 * n_sub
        tables = -(-sources // (256 // width))
        per_table = -(-sources // tables)
        blocks = dims + 2 * faces
        flat_rows = up_to(dims * m_pad + faces * j_pad + var_count, 128)
        vmem = pl.BlockSpec(memory_space=pltpu.VMEM)
        whole = pl.BlockSpec(memory_space=pltpu.HBM)
        moved = [
            jnp.transpose(dofs, (0, 2, 1)),
            stiffness,
            jnp.transpose(projection, (1, 0, 2)),
            jnp.transpose(star, (1, 2, 0, 3)),
            jnp.transpose(flux_minus, (1, 2, 0, 3)),
            jnp.transpose(flux_plus, (1, 2, 0, 3)),
            fault_flux,
        ]
        result = pl.pallas_call(
            functools.partial(kernel, (n_dom, n_sub)),
            out_shape=jax.ShapeDtypeStruct((var_count, elems, modes), F32),
            in_specs=[whole] * 7 + [vmem] * 4,
            out_specs=vmem,
            scratch_shapes=[pltpu.VMEM(one.shape, F32) for one in moved]
            + [
                pltpu.VMEM((var_count, dims, lanes), F32),
                pltpu.VMEM((var_count, faces, lanes), F32),
                pltpu.VMEM((var_count, faces, lanes), F32),
                pltpu.VMEM((up_to(var_count, 8), lanes), F32),
                pltpu.VMEM((16, lanes), jnp.int32),
                pltpu.VMEM((blocks, lanes, lanes), BF16),
                pltpu.VMEM((blocks, lanes, lanes), BF16),
                pltpu.VMEM((faces, faces, lanes, lanes), BF16),
                pltpu.VMEM((faces, lanes, width), BF16),
                pltpu.VMEM((tables, faces, per_table * width, lanes), BF16),
                pltpu.VMEM((flat_rows, 128), F32),
                pltpu.VMEM((m_pad, up_to(dims * m_pad, 128)), F32),
                pltpu.VMEM((up_to(lanes, 128), 128), F32),
                pltpu.VMEM((2, 8, 128), F32),
                pltpu.VMEM((2, sources, 8, 128), F32),
                pltpu.VMEM((tables, j_pad, per_table * width), F32),
                pltpu.SemaphoreType.DMA((len(moved),)),
                pltpu.SemaphoreType.DMA((2, sources - 1)),
                pltpu.SemaphoreType.DMA((2, sources - 1)),
            ],
            compiler_params=pltpu.CompilerParams(
                collective_id=0,
                has_side_effects=True,
                vmem_limit_bytes=67_043_328,
            ),
            name="window",
        )(
            *moved,
            fault_faces,
            levels.reshape(1, -1),
            face_source,
            send_source.reshape(1, -1),
        )
        return jnp.transpose(result, (0, 2, 1))

    return jax.shard_map(
        per_device,
        mesh=mesh,
        in_specs=(
            P(None, None, ("dom", "sub")),
            P(),
            P(),
            P(None, None, None, ("dom", "sub")),
            P(None, None, None, ("dom", "sub")),
            P(None, None, None, ("dom", "sub")),
            P(),
            P(None, ("dom", "sub")),
            P(("dom", "sub")),
            P(None, ("dom", "sub")),
            P(("dom", "sub")),
        ),
        out_specs=P(None, None, ("dom", "sub")),
        check_vma=False,
    )
```

```python
import functools
import math

import jax
import jax.numpy as jnp
from jax import lax
from jax.experimental import pallas as pl
from jax.experimental.pallas import tpu as pltpu
from jax.sharding import PartitionSpec as P

MESH = pl.DeviceIdType.MESH
ORDER = 6
fine_step = 0.75
F32 = jnp.float32
BF16 = jnp.bfloat16


def taylor_weights(start_time, stop_time, term_count):
    return [
        (stop_time ** (term + 1) - start_time ** (term + 1)) / math.factorial(term + 1)
        for term in range(term_count)
    ]


def up_to(value, step):
    return -(-value // step) * step


def dot(a, b):
    return jnp.dot(a, b, preferred_element_type=F32)


def split(value):
    high = value.astype(BF16)
    return high, (value - high.astype(F32)).astype(BF16)


def stacked(value):
    return jnp.concatenate(split(value), axis=0)


def halves(product):
    rows = product.shape[0] // 2
    return product[:rows] + product[rows:]


def left_product(left_both, right):
    high, low = split(right)
    rows = left_both.shape[0] // 2
    return halves(dot(left_both, high)) + dot(left_both[:rows], low)


def right_product(left_both, right_high, right_low):
    rows = left_both.shape[0] // 2
    return halves(dot(left_both, right_high)) + dot(left_both[:rows], right_low)


def kernel(
    sizes,
    dofs_hbm,
    stiffness_hbm,
    projection_hbm,
    star_hbm,
    minus_hbm,
    plus_hbm,
    fault_hbm,
    fault_faces,
    levels,
    face_source,
    send_source,
    out,
    dofs,
    stiffness,
    projection,
    star,
    flux_minus,
    flux_plus,
    fault_flux,
    star_rows,
    minus_rows,
    plus_rows,
    fault_rows,
    ints,
    block_high,
    block_low,
    picks,
    send_picks,
    remote_picks,
    flat,
    small,
    turn_ref,
    export,
    received,
    table_ref,
    load_sem,
    send_sem,
    recv_sem,
):
    n_dom, n_sub = sizes
    var_count, elems, modes = dofs.shape
    dims = stiffness.shape[0]
    face_modes, faces = projection.shape[0], projection.shape[1]
    slots = send_source.shape[1]
    lanes = var_count * elems
    m_pad = up_to(modes, 16)
    j_pad = up_to(face_modes, 16)
    groups = up_to(face_modes, 8) // 8
    width = var_count * slots
    sources = 3 * n_sub
    tables, _, table_lanes = table_ref.shape
    per_table = table_lanes // width

    loads = [
        pltpu.make_async_copy(src, dst, load_sem.at[i])
        for i, (src, dst) in enumerate(
            (
                (star_hbm, star),
                (dofs_hbm, dofs),
                (stiffness_hbm, stiffness),
                (projection_hbm, projection),
                (fault_hbm, fault_flux),
                (minus_hbm, flux_minus),
                (plus_hbm, flux_plus),
            )
        )
    ]
    for load in loads:
        load.start()

    me_dom, me_sub = lax.axis_index("dom"), lax.axis_index("sub")
    partners = []
    for delta in (-1, 0, 1):
        for turn in range(n_sub):
            if delta or turn:
                partners.append(
                    (
                        (
                            lax.rem(me_dom + delta + n_dom, n_dom),
                            lax.rem(me_sub + turn, n_sub),
                        ),
                        (1 - delta) * n_sub + me_sub,
                    )
                )
    barrier = pltpu.get_barrier_semaphore()
    for target, _ in partners:
        pl.semaphore_signal(barrier, inc=1, device_id=target, device_id_type=MESH)

    small[...] = jnp.zeros_like(small)
    flat[...] = jnp.zeros_like(flat)
    turn_ref[...] = jnp.zeros_like(turn_ref)
    table_ref[...] = jnp.zeros_like(table_ref)
    export[...] = jnp.zeros_like(export)

    mask = (
        lax.broadcasted_iota(jnp.int32, (elems, lanes), 1) % elems
        == lax.broadcasted_iota(jnp.int32, (elems, lanes), 0)
    )

    def spread(rows, f, i):
        for w in range(var_count):
            row = rows[w, f : f + 1, :]
            high = row.astype(BF16).astype(F32)
            low = row - high
            at = slice(w * elems, (w + 1) * elems)
            block_high[i, at, :] = jnp.where(mask, high, 0.0).astype(BF16)
            block_low[i, at, :] = jnp.where(mask, low, 0.0).astype(BF16)

    send_row = send_source[...]
    for i in range(width // slots):
        ints[9:10, i * slots : (i + 1) * slots] = send_row
    for v in range(var_count):
        at = slice(v * elems, (v + 1) * elems)
        ints[0:faces, at] = face_source[...]
        ints[4 : 4 + faces, at] = fault_faces[...]
        ints[8:9, at] = levels[...]

    def code(shape, dim, element_count):
        index = lax.broadcasted_iota(jnp.int32, shape, dim)
        return index // element_count, index % element_count

    row_var, row_elem = code((lanes, width), 0, elems)
    lane_var, _ = code((lanes, width), 1, slots)
    send_key = jnp.where(row_var == lane_var, row_elem, -(2**20))
    for f in range(faces):
        send_picks[f] = jnp.where(
            send_key == ints[9:10, 0:width] - f * elems, 1.0, 0.0
        ).astype(BF16)

    row_var, row_elem = code((lanes, lanes), 0, elems)
    lane_var, _ = code((lanes, lanes), 1, elems)
    key = jnp.where(row_var == lane_var, row_elem, -(2**20))
    source_id, inside = code((table_lanes, lanes), 0, width)
    slot_var, slot = inside // slots, inside % slots
    lane_var, _ = code((table_lanes, lanes), 1, elems)
    remote_key = jnp.where(
        slot_var == lane_var, faces * elems + source_id * slots + slot, -(2**20)
    )
    for f in range(faces):
        wanted = ints[f : f + 1, :]
        for g in range(faces):
            picks[g, f] = jnp.where(key == wanted - g * elems, 1.0, 0.0).astype(BF16)
        for t in range(tables):
            remote_picks[t, f] = jnp.where(
                remote_key == wanted - t * per_table * slots, 1.0, 0.0
            ).astype(BF16)

    loads[0].wait()
    for v in range(var_count):
        star_rows[:, :, v * elems : (v + 1) * elems] = star[v]
    for d in range(dims):
        spread(star_rows, d, d)

    loads[1].wait()
    turn_ref[0:lanes, 0:modes] = dofs[...].reshape(lanes, modes)
    state = jnp.transpose(turn_ref[...])[0:m_pad, 0:lanes]

    loads[2].wait()
    for d in range(dims):
        small[0:modes, d * m_pad : d * m_pad + modes] = stiffness[d]
    forward = stacked(small[0:m_pad, 0 : dims * m_pad])

    def turned(value):
        both = stacked(value)
        return [
            right_product(both, block_high[d], block_low[d]) for d in range(dims)
        ]

    def series(value, weight_sets):
        totals = [weights[0] * value for weights in weight_sets]
        for term in range(1, ORDER):
            value = left_product(forward, jnp.concatenate(turned(value), axis=0))
            totals = [
                total + weights[term] * value
                for total, weights in zip(totals, weight_sets)
            ]
        return totals

    first_weights = taylor_weights(0.0, fine_step, ORDER)
    second_weights = taylor_weights(fine_step, 2.0 * fine_step, ORDER)

    loads[3].wait()
    loads[4].wait()
    for d in range(dims):
        flat[d * m_pad : d * m_pad + modes, 0:modes] = stiffness[d]
    base = dims * m_pad
    for f in range(faces):
        flat[base + f * j_pad : base + f * j_pad + face_modes, 0:modes] = -projection[
            :, f, :
        ]
    base_fault = base + faces * j_pad
    flat[base_fault : base_fault + var_count, 0:var_count] = fault_flux[...]

    first_half, second_half = series(state, (first_weights, second_weights))

    project = stacked(-flat[base : base + faces * j_pad, 0:m_pad])

    def face_halves(value):
        both = stacked(left_product(project, value))
        count = faces * j_pad
        return [
            jnp.concatenate(
                [
                    both[f * j_pad : (f + 1) * j_pad],
                    both[count + f * j_pad : count + (f + 1) * j_pad],
                ],
                axis=0,
            )
            for f in range(faces)
        ]

    def total_of(parts):
        return functools.reduce(lambda a, b: a + b, parts)

    own_slot = n_sub + me_sub

    def launch(phase, face_parts):
        block = halves(
            total_of([dot(face_parts[f], send_picks[f]) for f in range(faces)])
        )
        for g in range(groups):
            export[phase, :, g * width : (g + 1) * width] = block[8 * g : 8 * g + 8]
        copies = []
        for i, (target, slot) in enumerate(partners):
            copy = pltpu.make_async_remote_copy(
                src_ref=export.at[phase],
                dst_ref=received.at[phase, slot],
                send_sem=send_sem.at[phase, i],
                recv_sem=recv_sem.at[phase, i],
                device_id=target,
                device_id_type=MESH,
            )
            copy.start()
            copies.append(copy)
        received[phase, own_slot] = export[phase]
        return copies

    def local_part(value, face_parts):
        volume = turned(value)
        own = [
            right_product(face_parts[f], block_high[dims + f], block_low[dims + f])
            for f in range(faces)
        ]
        beside = [
            total_of([dot(face_parts[g], picks[g, f]) for g in range(faces)])
            for f in range(faces)
        ]
        return volume, own, beside

    def finish(phase, copies, parts, back):
        volume, own, beside = parts
        for copy in copies:
            copy.wait_recv()
        for k in range(sources):
            t, at = k // per_table, k % per_table * width
            for g in range(groups):
                table_ref[t, 8 * g : 8 * g + 8, at : at + width] = received[
                    phase, k, :, g * width : (g + 1) * width
                ]
        table_parts = [stacked(table_ref[t]) for t in range(tables)]
        flux = []
        for f in range(faces):
            gathered = halves(
                beside[f]
                + total_of([dot(table_parts[t], remote_picks[t, f]) for t in range(tables)])
            )
            at = dims + faces + f
            flux.append(
                own[f] + right_product(stacked(gathered), block_high[at], block_low[at])
            )
        return left_product(back, jnp.concatenate(volume + flux, axis=0))

    face_parts = face_halves(first_half)
    pl.semaphore_wait(barrier, len(partners))
    copies = launch(0, face_parts)

    flipped = jnp.transpose(flat[...])
    back = stacked(flipped[0:m_pad, 0:base_fault])
    loads[5].wait()
    loads[6].wait()
    for v in range(var_count):
        at = slice(v * elems, (v + 1) * elems)
        minus_rows[:, :, at] = flux_minus[v]
        plus_rows[:, :, at] = flux_plus[v]
        fault_rows[0:var_count, at] = jnp.broadcast_to(
            flipped[0:var_count, base_fault + v : base_fault + v + 1], (var_count, elems)
        )
    on_fault = ints[4 : 4 + faces, :] == 1
    for w in range(var_count):
        plus_rows[w] = jnp.where(on_fault, fault_rows[w : w + 1, :], plus_rows[w])
    for f in range(faces):
        spread(minus_rows, f, dims + f)
        spread(plus_rows, f, dims + faces + f)
    parts = local_part(first_half, face_parts)
    moved = state + finish(0, copies, parts, back)
    (fine_half,) = series(moved, (first_weights,))
    carried = jnp.where(ints[8:9, :] == 0, fine_half, second_half)
    face_parts = face_halves(carried)
    last_copies = launch(1, face_parts)
    parts = local_part(carried, face_parts)
    result = moved + finish(1, last_copies, parts, back)
    turned_back = jnp.transpose(
        jnp.concatenate(
            [
                jnp.concatenate(
                    [result, jnp.zeros((m_pad, turn_ref.shape[0] - lanes), F32)], axis=1
                ),
                jnp.zeros((128 - m_pad, turn_ref.shape[0]), F32),
            ],
            axis=0,
        )
    )
    out[...] = turned_back[0:lanes, 0:modes].reshape(var_count, elems, modes)
    for copy in copies + last_copies:
        copy.wait_send()


def solution(mesh):
    n_dom, n_sub = mesh.shape["dom"], mesh.shape["sub"]

    def per_device(
        dofs,
        stiffness,
        projection,
        star,
        flux_minus,
        flux_plus,
        fault_flux,
        fault_faces,
        levels,
        face_source,
        send_source,
    ):
        var_count, modes, elems = dofs.shape
        dims = stiffness.shape[0]
        faces, face_modes = projection.shape[0], projection.shape[1]
        slots = send_source.shape[0]
        lanes = var_count * elems
        m_pad, j_pad = up_to(modes, 16), up_to(face_modes, 16)
        width = var_count * slots
        sources = 3 * n_sub
        tables = -(-sources // (256 // width))
        per_table = -(-sources // tables)
        blocks = dims + 2 * faces
        flat_rows = up_to(dims * m_pad + faces * j_pad + var_count, 128)
        vmem = pl.BlockSpec(memory_space=pltpu.VMEM)
        whole = pl.BlockSpec(memory_space=pltpu.HBM)
        moved = [
            jnp.transpose(dofs, (0, 2, 1)),
            stiffness,
            jnp.transpose(projection, (1, 0, 2)),
            jnp.transpose(star, (1, 2, 0, 3)),
            jnp.transpose(flux_minus, (1, 2, 0, 3)),
            jnp.transpose(flux_plus, (1, 2, 0, 3)),
            fault_flux,
        ]
        result = pl.pallas_call(
            functools.partial(kernel, (n_dom, n_sub)),
            out_shape=pltpu.VMEM((var_count, elems, modes), F32),
            in_specs=[whole] * 7 + [vmem] * 4,
            out_specs=vmem,
            scratch_shapes=[pltpu.VMEM(one.shape, F32) for one in moved]
            + [
                pltpu.VMEM((var_count, dims, lanes), F32),
                pltpu.VMEM((var_count, faces, lanes), F32),
                pltpu.VMEM((var_count, faces, lanes), F32),
                pltpu.VMEM((up_to(var_count, 8), lanes), F32),
                pltpu.VMEM((16, lanes), jnp.int32),
                pltpu.VMEM((blocks, lanes, lanes), BF16),
                pltpu.VMEM((blocks, lanes, lanes), BF16),
                pltpu.VMEM((faces, faces, lanes, lanes), BF16),
                pltpu.VMEM((faces, lanes, width), BF16),
                pltpu.VMEM((tables, faces, per_table * width, lanes), BF16),
                pltpu.VMEM((flat_rows, 128), F32),
                pltpu.VMEM((m_pad, up_to(dims * m_pad, 128)), F32),
                pltpu.VMEM((up_to(lanes, 128), 128), F32),
                pltpu.VMEM((2, 8, 128), F32),
                pltpu.VMEM((2, sources, 8, 128), F32),
                pltpu.VMEM((tables, j_pad, per_table * width), F32),
                pltpu.SemaphoreType.DMA((len(moved),)),
                pltpu.SemaphoreType.DMA((2, sources - 1)),
                pltpu.SemaphoreType.DMA((2, sources - 1)),
            ],
            compiler_params=pltpu.CompilerParams(
                collective_id=0,
                has_side_effects=True,
                vmem_limit_bytes=66_000_000,
            ),
            name="window",
        )(
            *moved,
            fault_faces,
            levels.reshape(1, -1),
            face_source,
            send_source.reshape(1, -1),
        )
        return jnp.transpose(result, (0, 2, 1))

    return jax.shard_map(
        per_device,
        mesh=mesh,
        in_specs=(
            P(None, None, ("dom", "sub")),
            P(),
            P(),
            P(None, None, None, ("dom", "sub")),
            P(None, None, None, ("dom", "sub")),
            P(None, None, None, ("dom", "sub")),
            P(),
            P(None, ("dom", "sub")),
            P(("dom", "sub")),
            P(None, ("dom", "sub")),
            P(("dom", "sub")),
        ),
        out_specs=P(None, None, ("dom", "sub")),
        check_vma=False,
    )
```

```python
import functools
import math

import jax
import jax.numpy as jnp
from jax import lax
from jax.experimental import pallas as pl
from jax.experimental.pallas import tpu as pltpu
from jax.sharding import PartitionSpec as P

MESH = pl.DeviceIdType.MESH
ORDER = 6
fine_step = 0.75
F32 = jnp.float32
BF16 = jnp.bfloat16


def taylor_weights(start_time, stop_time, term_count):
    return [
        (stop_time ** (term + 1) - start_time ** (term + 1)) / math.factorial(term + 1)
        for term in range(term_count)
    ]


def up_to(value, step):
    return -(-value // step) * step


def dot(a, b):
    return jnp.dot(a, b, preferred_element_type=F32)


def split(value):
    high = value.astype(BF16)
    return high, (value - high.astype(F32)).astype(BF16)


def stacked(value):
    return jnp.concatenate(split(value), axis=0)


def halves(product):
    rows = product.shape[0] // 2
    return product[:rows] + product[rows:]


def left_product(left_both, right):
    high, low = split(right)
    rows = left_both.shape[0] // 2
    return halves(dot(left_both, high)) + dot(left_both[:rows], low)


def right_product(left_both, right_high, right_low):
    rows = left_both.shape[0] // 2
    return halves(dot(left_both, right_high)) + dot(left_both[:rows], right_low)


def kernel(
    sizes,
    dofs_hbm,
    stiffness_hbm,
    projection_hbm,
    star_hbm,
    minus_hbm,
    plus_hbm,
    fault_hbm,
    fault_faces,
    levels,
    face_source,
    send_source,
    out,
    dofs,
    stiffness,
    projection,
    star,
    flux_minus,
    flux_plus,
    fault_flux,
    star_rows,
    minus_rows,
    plus_rows,
    fault_rows,
    ints,
    block_high,
    block_low,
    picks,
    send_picks,
    remote_picks,
    flat,
    small,
    turn_ref,
    export,
    received,
    table_ref,
    load_sem,
    send_sem,
    recv_sem,
):
    n_dom, n_sub = sizes
    var_count, elems, modes = dofs.shape
    dims = stiffness.shape[0]
    face_modes, faces = projection.shape[0], projection.shape[1]
    slots = send_source.shape[1]
    lanes = var_count * elems
    m_pad = up_to(modes, 16)
    j_pad = up_to(face_modes, 16)
    groups = up_to(face_modes, 8) // 8
    width = var_count * slots
    sources = 3 * n_sub
    tables, _, table_lanes = table_ref.shape
    per_table = table_lanes // width

    loads = [
        pltpu.make_async_copy(src, dst, load_sem.at[i])
        for i, (src, dst) in enumerate(
            (
                (star_hbm, star),
                (dofs_hbm, dofs),
                (stiffness_hbm, stiffness),
                (projection_hbm, projection),
                (fault_hbm, fault_flux),
                (minus_hbm, flux_minus),
                (plus_hbm, flux_plus),
            )
        )
    ]
    for load in loads:
        load.start()

    me_dom, me_sub = lax.axis_index("dom"), lax.axis_index("sub")
    partners = []
    for delta in (-1, 0, 1):
        for turn in range(n_sub):
            if delta or turn:
                partners.append(
                    (
                        (
                            lax.rem(me_dom + delta + n_dom, n_dom),
                            lax.rem(me_sub + turn, n_sub),
                        ),
                        (1 - delta) * n_sub + me_sub,
                    )
                )
    barrier = pltpu.get_barrier_semaphore()
    for target, _ in partners:
        pl.semaphore_signal(barrier, inc=1, device_id=target, device_id_type=MESH)

    small[...] = jnp.zeros_like(small)
    flat[...] = jnp.zeros_like(flat)
    turn_ref[...] = jnp.zeros_like(turn_ref)
    table_ref[...] = jnp.zeros_like(table_ref)
    export[...] = jnp.zeros_like(export)

    mask = (
        lax.broadcasted_iota(jnp.int32, (elems, lanes), 1) % elems
        == lax.broadcasted_iota(jnp.int32, (elems, lanes), 0)
    )

    def spread(rows, f, i):
        for w in range(var_count):
            row = rows[w, f : f + 1, :]
            high = row.astype(BF16).astype(F32)
            low = row - high
            at = slice(w * elems, (w + 1) * elems)
            block_high[i, at, :] = jnp.where(mask, high, 0.0).astype(BF16)
            block_low[i, at, :] = jnp.where(mask, low, 0.0).astype(BF16)

    send_row = send_source[...]
    for i in range(width // slots):
        ints[9:10, i * slots : (i + 1) * slots] = send_row
    for v in range(var_count):
        at = slice(v * elems, (v + 1) * elems)
        ints[0:faces, at] = face_source[...]
        ints[4 : 4 + faces, at] = fault_faces[...]
        ints[8:9, at] = levels[...]

    def code(shape, dim, element_count):
        index = lax.broadcasted_iota(jnp.int32, shape, dim)
        return index // element_count, index % element_count

    row_var, row_elem = code((lanes, width), 0, elems)
    lane_var, _ = code((lanes, width), 1, slots)
    send_key = jnp.where(row_var == lane_var, row_elem, -(2**20))
    for f in range(faces):
        send_picks[f] = jnp.where(
            send_key == ints[9:10, 0:width] - f * elems, 1.0, 0.0
        ).astype(BF16)

    row_var, row_elem = code((lanes, lanes), 0, elems)
    lane_var, _ = code((lanes, lanes), 1, elems)
    key = jnp.where(row_var == lane_var, row_elem, -(2**20))
    source_id, inside = code((table_lanes, lanes), 0, width)
    slot_var, slot = inside // slots, inside % slots
    lane_var, _ = code((table_lanes, lanes), 1, elems)
    remote_key = jnp.where(
        slot_var == lane_var, faces * elems + source_id * slots + slot, -(2**20)
    )
    for f in range(faces):
        wanted = ints[f : f + 1, :]
        for g in range(faces):
            picks[g, f] = jnp.where(key == wanted - g * elems, 1.0, 0.0).astype(BF16)
        for t in range(tables):
            remote_picks[t, f] = jnp.where(
                remote_key == wanted - t * per_table * slots, 1.0, 0.0
            ).astype(BF16)

    loads[0].wait()
    for v in range(var_count):
        star_rows[:, :, v * elems : (v + 1) * elems] = star[v]
    for d in range(dims):
        spread(star_rows, d, d)

    loads[1].wait()
    turn_ref[0:lanes, 0:modes] = dofs[...].reshape(lanes, modes)
    state = jnp.transpose(turn_ref[...])[0:m_pad, 0:lanes]

    loads[2].wait()
    for d in range(dims):
        small[0:modes, d * m_pad : d * m_pad + modes] = stiffness[d]
    forward = stacked(small[0:m_pad, 0 : dims * m_pad])

    def turned(value):
        both = stacked(value)
        return [
            right_product(both, block_high[d], block_low[d]) for d in range(dims)
        ]

    def series(value, weight_sets):
        totals = [weights[0] * value for weights in weight_sets]
        for term in range(1, ORDER):
            value = left_product(forward, jnp.concatenate(turned(value), axis=0))
            totals = [
                total + weights[term] * value
                for total, weights in zip(totals, weight_sets)
            ]
        return totals

    first_weights = taylor_weights(0.0, fine_step, ORDER)
    second_weights = taylor_weights(fine_step, 2.0 * fine_step, ORDER)

    loads[3].wait()
    loads[4].wait()
    for d in range(dims):
        flat[d * m_pad : d * m_pad + modes, 0:modes] = stiffness[d]
    base = dims * m_pad
    for f in range(faces):
        flat[base + f * j_pad : base + f * j_pad + face_modes, 0:modes] = -projection[
            :, f, :
        ]
    base_fault = base + faces * j_pad
    flat[base_fault : base_fault + var_count, 0:var_count] = fault_flux[...]

    first_half, second_half = series(state, (first_weights, second_weights))

    project = stacked(-flat[base : base + faces * j_pad, 0:m_pad])

    def face_halves(value):
        both = stacked(left_product(project, value))
        count = faces * j_pad
        return [
            jnp.concatenate(
                [
                    both[f * j_pad : (f + 1) * j_pad],
                    both[count + f * j_pad : count + (f + 1) * j_pad],
                ],
                axis=0,
            )
            for f in range(faces)
        ]

    def total_of(parts):
        return functools.reduce(lambda a, b: a + b, parts)

    own_slot = n_sub + me_sub

    def launch(phase, face_parts):
        block = halves(
            total_of([dot(face_parts[f], send_picks[f]) for f in range(faces)])
        )
        for g in range(groups):
            export[phase, :, g * width : (g + 1) * width] = block[8 * g : 8 * g + 8]
        copies = []
        for i, (target, slot) in enumerate(partners):
            copy = pltpu.make_async_remote_copy(
                src_ref=export.at[phase],
                dst_ref=received.at[phase, slot],
                send_sem=send_sem.at[phase, i],
                recv_sem=recv_sem.at[phase, i],
                device_id=target,
                device_id_type=MESH,
            )
            copy.start()
            copies.append(copy)
        received[phase, own_slot] = export[phase]
        return copies

    def local_part(value, face_parts, back):
        volume = turned(value)
        own = [
            right_product(face_parts[f], block_high[dims + f], block_low[dims + f])
            for f in range(faces)
        ]
        beside = [
            total_of([dot(face_parts[g], picks[g, f]) for g in range(faces)])
            for f in range(faces)
        ]
        flux = [
            own[f]
            + right_product(
                stacked(halves(beside[f])),
                block_high[dims + faces + f],
                block_low[dims + faces + f],
            )
            for f in range(faces)
        ]
        return left_product(back, jnp.concatenate(volume + flux, axis=0))

    def finish(phase, copies, parts, back):
        for copy in copies:
            copy.wait_recv()
        for k in range(sources):
            t, at = k // per_table, k % per_table * width
            for g in range(groups):
                table_ref[t, 8 * g : 8 * g + 8, at : at + width] = received[
                    phase, k, :, g * width : (g + 1) * width
                ]
        table_parts = [stacked(table_ref[t]) for t in range(tables)]
        flux = []
        for f in range(faces):
            gathered = halves(
                total_of([dot(table_parts[t], remote_picks[t, f]) for t in range(tables)])
            )
            at = dims + faces + f
            flux.append(
                right_product(stacked(gathered), block_high[at], block_low[at])
            )
        return parts + left_product(back[:, base:], jnp.concatenate(flux, axis=0))

    face_parts = face_halves(first_half)
    pl.semaphore_wait(barrier, len(partners))
    copies = launch(0, face_parts)

    flipped = jnp.transpose(flat[...])
    back = stacked(flipped[0:m_pad, 0:base_fault])
    loads[5].wait()
    loads[6].wait()
    for v in range(var_count):
        at = slice(v * elems, (v + 1) * elems)
        minus_rows[:, :, at] = flux_minus[v]
        plus_rows[:, :, at] = flux_plus[v]
        fault_rows[0:var_count, at] = jnp.broadcast_to(
            flipped[0:var_count, base_fault + v : base_fault + v + 1], (var_count, elems)
        )
    on_fault = ints[4 : 4 + faces, :] == 1
    for w in range(var_count):
        plus_rows[w] = jnp.where(on_fault, fault_rows[w : w + 1, :], plus_rows[w])
    for f in range(faces):
        spread(minus_rows, f, dims + f)
        spread(plus_rows, f, dims + faces + f)
    parts = local_part(first_half, face_parts, back)
    moved = state + finish(0, copies, parts, back)
    (fine_half,) = series(moved, (first_weights,))
    carried = jnp.where(ints[8:9, :] == 0, fine_half, second_half)
    face_parts = face_halves(carried)
    last_copies = launch(1, face_parts)
    parts = local_part(carried, face_parts, back)
    result = moved + finish(1, last_copies, parts, back)
    turned_back = jnp.transpose(
        jnp.concatenate(
            [
                jnp.concatenate(
                    [result, jnp.zeros((m_pad, turn_ref.shape[0] - lanes), F32)], axis=1
                ),
                jnp.zeros((128 - m_pad, turn_ref.shape[0]), F32),
            ],
            axis=0,
        )
    )
    out[...] = turned_back[0:lanes, 0:modes].reshape(var_count, elems, modes)
    for copy in copies + last_copies:
        copy.wait_send()


def solution(mesh):
    n_dom, n_sub = mesh.shape["dom"], mesh.shape["sub"]

    def per_device(
        dofs,
        stiffness,
        projection,
        star,
        flux_minus,
        flux_plus,
        fault_flux,
        fault_faces,
        levels,
        face_source,
        send_source,
    ):
        var_count, modes, elems = dofs.shape
        dims = stiffness.shape[0]
        faces, face_modes = projection.shape[0], projection.shape[1]
        slots = send_source.shape[0]
        lanes = var_count * elems
        m_pad, j_pad = up_to(modes, 16), up_to(face_modes, 16)
        width = var_count * slots
        sources = 3 * n_sub
        tables = -(-sources // (256 // width))
        per_table = -(-sources // tables)
        blocks = dims + 2 * faces
        flat_rows = up_to(dims * m_pad + faces * j_pad + var_count, 128)
        vmem = pl.BlockSpec(memory_space=pltpu.VMEM)
        whole = pl.BlockSpec(memory_space=pltpu.HBM)
        moved = [
            jnp.transpose(dofs, (0, 2, 1)),
            stiffness,
            jnp.transpose(projection, (1, 0, 2)),
            jnp.transpose(star, (1, 2, 0, 3)),
            jnp.transpose(flux_minus, (1, 2, 0, 3)),
            jnp.transpose(flux_plus, (1, 2, 0, 3)),
            fault_flux,
        ]
        result = pl.pallas_call(
            functools.partial(kernel, (n_dom, n_sub)),
            out_shape=pltpu.VMEM((var_count, elems, modes), F32),
            in_specs=[whole] * 7 + [vmem] * 4,
            out_specs=vmem,
            scratch_shapes=[pltpu.VMEM(one.shape, F32) for one in moved]
            + [
                pltpu.VMEM((var_count, dims, lanes), F32),
                pltpu.VMEM((var_count, faces, lanes), F32),
                pltpu.VMEM((var_count, faces, lanes), F32),
                pltpu.VMEM((up_to(var_count, 8), lanes), F32),
                pltpu.VMEM((16, lanes), jnp.int32),
                pltpu.VMEM((blocks, lanes, lanes), BF16),
                pltpu.VMEM((blocks, lanes, lanes), BF16),
                pltpu.VMEM((faces, faces, lanes, lanes), BF16),
                pltpu.VMEM((faces, lanes, width), BF16),
                pltpu.VMEM((tables, faces, per_table * width, lanes), BF16),
                pltpu.VMEM((flat_rows, 128), F32),
                pltpu.VMEM((m_pad, up_to(dims * m_pad, 128)), F32),
                pltpu.VMEM((up_to(lanes, 128), 128), F32),
                pltpu.VMEM((2, 8, 128), F32),
                pltpu.VMEM((2, sources, 8, 128), F32),
                pltpu.VMEM((tables, j_pad, per_table * width), F32),
                pltpu.SemaphoreType.DMA((len(moved),)),
                pltpu.SemaphoreType.DMA((2, sources - 1)),
                pltpu.SemaphoreType.DMA((2, sources - 1)),
            ],
            compiler_params=pltpu.CompilerParams(
                collective_id=0,
                has_side_effects=True,
                vmem_limit_bytes=66_000_000,
            ),
            name="window",
        )(
            *moved,
            fault_faces,
            levels.reshape(1, -1),
            face_source,
            send_source.reshape(1, -1),
        )
        return jnp.transpose(result, (0, 2, 1))

    return jax.shard_map(
        per_device,
        mesh=mesh,
        in_specs=(
            P(None, None, ("dom", "sub")),
            P(),
            P(),
            P(None, None, None, ("dom", "sub")),
            P(None, None, None, ("dom", "sub")),
            P(None, None, None, ("dom", "sub")),
            P(),
            P(None, ("dom", "sub")),
            P(("dom", "sub")),
            P(None, ("dom", "sub")),
            P(("dom", "sub")),
        ),
        out_specs=P(None, None, ("dom", "sub")),
        check_vma=False,
    )
```
